32 devices in a mesh: row: 4 (over y, x), col: 8 (over z, core).
Axes of the slice: x: 2, y: 2, z: 4, core: 2. Of those that a mesh axis runs over, the one named last changes fastest.
Arguments:
- charge: float32 [256, 256, 256], P('col', 'row'), may hold values from -6 to 6
- green_spectrum: float32 [512, 512, 512], P('row', 'col'), may hold values from 0.2 to 2
Outputs:
- potential: float32 [256, 256, 256], P('col', 'row')
The draws below stay inside these ranges and needn't reach their ends.
All inputs are finite; a program needn't handle non-finite values.
Results may differ from the reference program's by a relative error of at most 0.00007.
Values sent between devices are 32-bit elements; how exact they have to be, the bound alone decides.
A program may use at most 192 MiB of HBM per device.

```python
import math
import jax
import jax.numpy as jnp

M = 512
N = 256


def block_levels(key, shape, shards, low, largest):
    gain, own = 1.0, jax.random.fold_in(key, 6)
    for axis_at, blocks in shards:
        heights = jnp.exp(jax.random.uniform(jax.random.fold_in(own, axis_at), (blocks,), jnp.float32, low / len(shards), largest / len(shards)))
        gain = gain * jnp.repeat(heights, shape[axis_at] // blocks).reshape([-1 if axis == axis_at else 1 for axis in range(len(shape))])
    return gain


def noise(rng, dims, spread, bound, shards=(), held_as=jnp.bfloat16):
    array = jax.random.normal(rng, dims, jnp.float32) * spread
    if len(shards) > 0:
        array = block_levels(rng, dims, shards, -0.22, 0.18) * array
    return jnp.clip(array, min=-bound, max=bound).astype(held_as)


def setup_inputs(seed: int = 0) -> dict:
    seeds = jax.random.split(jax.random.key(seed), 3)
    charge = noise(seeds[0], (N, N, N), 1.0, 6.0, ((0, 8), (1, 4)), jnp.float32)
    green_spectrum = jnp.clip(jnp.exp(math.log(2.0) - 2.3025851 * jax.random.uniform(seeds[1], (M, M, M), jnp.float32) ** block_levels(seeds[1], (M, M, M), ((0, 4), (1, 8)), -0.2, 0.2)), 0.2, 2.0)
    return {"charge": charge, "green_spectrum": green_spectrum}


def reference(charge, green_spectrum):
    spectrum = jnp.fft.fft(charge, n=M, axis=2)
    spectrum = jnp.fft.fft(spectrum, n=M, axis=1)
    spectrum = jnp.fft.fft(spectrum, n=M, axis=0)
    product = spectrum * jnp.transpose(green_spectrum, (2, 1, 0))
    field = jnp.fft.ifft(product, axis=0)[:N]
    field = jnp.fft.ifft(field, axis=1)[:, :N]
    field = jnp.fft.ifft(field, axis=2)[:, :, :N]
    return jnp.real(field).astype(jnp.float32)
```

```python
import math

import jax
import jax.numpy as jnp
from jax import lax
from jax.sharding import PartitionSpec as P

M = 512
N = 256


def phases(count_in, count_out, length):
    row_ids = lax.iota(jnp.int32, count_in)[:, None]
    col_ids = lax.iota(jnp.int32, count_out)[None, :]
    turn_ids = row_ids * col_ids % length
    angles = turn_ids.astype(jnp.float32) * (2.0 * math.pi / length)
    return (jnp.cos(angles), jnp.sin(angles))


def forward_table(count_in, count_out, length):
    cosine, sine_part = phases(count_in, count_out, length)
    return jnp.stack([jnp.stack([cosine, -sine_part], 1), jnp.stack([sine_part, cosine], 1)], 0)


def inverse_table(count_in, count_out, length):
    cosine, sine_part = phases(count_in, count_out, length)
    scaling = 1.0 / length
    return (
        jnp.stack([jnp.stack([cosine, sine_part], 1), jnp.stack([-sine_part, cosine], 1)], 0)
        * scaling
    )


def contract(pattern, left_side, right_side):
    return jnp.einsum(
        pattern,
        left_side,
        right_side,
        precision=lax.Precision.HIGH,
        preferred_element_type=jnp.float32,
    )


def on_device(charge, green_spectrum):
    cosine, sine_part = phases(N, M, M)
    real_table = jnp.stack([cosine, -sine_part], 1)
    along_z = contract("xyz,zqk->xyqk", charge, real_table)
    by_rows = lax.all_to_all(along_z, "row", split_axis=3, concat_axis=1, tiled=True)
    forward = forward_table(N, M, M)
    along_y = contract("xypk,pyqb->xkqb", by_rows, forward)
    spectrum = contract(
        "xkpj,pxqa->kjqa",
        lax.all_to_all(along_y, "col", split_axis=3, concat_axis=0, tiled=True),
        forward,
    )
    product = spectrum * green_spectrum[:, :, None, :]
    back_table = inverse_table(M, N, M)
    back_cos, back_sin = phases(M, N, M)
    real_back = jnp.stack([back_cos, -back_sin], 0) * (1.0 / M)
    back_x = contract("kjqa,qapx->kjpx", product, back_table)
    by_cols = lax.all_to_all(back_x, "col", split_axis=3, concat_axis=1, tiled=True)
    back_y = contract("kbpx,pbqy->kxqy", by_cols, back_table)
    return contract(
        "cxpy,pcz->xyz",
        lax.all_to_all(back_y, "row", split_axis=3, concat_axis=0, tiled=True),
        real_back,
    )


def solution(mesh):
    in_specs = (P("col", "row", None), P("row", "col", None))
    out_specs = P("col", "row", None)
    return jax.shard_map(
        on_device, mesh=mesh, in_specs=in_specs, out_specs=out_specs, check_vma=False
    )
```
